32 devices in a mesh: cols: 8 (over z, y), rows: 4 (over x, core).
Axes of the slice: x: 2, y: 2, z: 4, core: 2. Of those that a mesh axis runs over, the one named last changes fastest.
Arguments:
- gradient: bfloat16 [8192, 28672], P('rows', 'cols'), may hold values from -6 to 6
- eigenbasis: float32 [8192, 8192], P('rows', 'cols'), may hold values from -0.0625 to 0.0625
- first_moment: float32 [4, 256, 28672], P(None, 'rows', 'cols'), may hold values from -4 to 4
- second_moment: float32 [4, 256, 28672], P(None, 'rows', 'cols'), may hold values from 0.2 to 2
- prior_update: float32 [8192, 28672], P('rows', 'cols'), may hold values from -3 to 3
- group_ids: int32 [4], replicated, may hold values from 0 to 31, as said below
Outputs:
- first_out: float32 [4, 256, 28672], P(None, 'rows', 'cols')
- second_out: float32 [4, 256, 28672], P(None, 'rows', 'cols')
- update: float32 [8192, 28672], P('rows', 'cols')
The draws below stay inside these ranges and needn't reach their ends.
Inputs may be any that keep to these rules, and one draw needn't show every extreme that they name: `group_ids`: the 4 entries are distinct.
All inputs are finite; a program needn't handle non-finite values.
Results may differ from the reference program's by a relative error of at most 0.0003.
Values sent between devices are 32-bit elements; how exact they have to be, the bound alone decides.
No kernel may reach another device: no remote copies, remote signals or barrier semaphores. Data moves between devices by JAX's collectives and lax.ppermute only.
A program may use at most 256 MiB of HBM per device.

```python
import math
import jax
import jax.numpy as jnp
from jax import lax

M = 8192
N = 28672
GROUP = 256
GROUPS = 4


def draw_group_ids(key, part):
    blocks = M // GROUP
    inner = jax.random.permutation(jax.random.fold_in(key, 7), blocks - 2) + 1
    chosen = jnp.concatenate([jnp.array([0, blocks - 1], jnp.int32), inner[:GROUPS - 2].astype(jnp.int32)])
    order = jax.random.permutation(jax.random.fold_in(key, 11), GROUPS)
    return chosen[order].astype(jnp.int32)


def levels(rng, extent, shards, low, top_value):
    def one(position, parts):
        draws = jax.random.uniform(jax.random.fold_in(jax.random.fold_in(rng, 6), position), (parts,), jnp.float32, low / len(shards), top_value / len(shards))
        return jnp.repeat(jnp.exp(draws), extent[position] // parts).reshape((-1,) + (1,) * (len(extent) - position - 1))

    level = one(*shards[0])
    for cut in shards[1:]:
        level = level * one(*cut)
    return level


def noise(key, extent, width, limit, shards=(), held_as=jnp.bfloat16):
    gain = levels(key, extent, shards, -0.22, 0.18) if shards else 1.0
    drawn = jax.random.normal(key, extent, jnp.float32) * width * gain
    return jnp.minimum(jnp.maximum(drawn, -limit), limit).astype(held_as)


def setup_inputs(seed: int = 0) -> dict:
    key_list = jax.random.split(jax.random.key(seed), 7)
    gradient = noise(key_list[0], (M, N), 1.0, 6.0, ((0, 4), (1, 8)))
    eigenbasis = noise(key_list[1], (M, M), M ** -0.5, 0.0625, ((0, 4), (1, 8)), jnp.float32)
    first_moment = noise(key_list[2], (GROUPS, GROUP, N), 0.5, 4.0, ((1, 4), (2, 8)), jnp.float32)
    second_moment = jnp.clip(jnp.exp(math.log(2.0) - 2.3025851 * jax.random.uniform(key_list[3], (GROUPS, GROUP, N), jnp.float32) ** levels(key_list[3], (GROUPS, GROUP, N), ((1, 4), (2, 8)), -0.2, 0.2)), 0.2, 2.0)
    prior_update = noise(key_list[4], (M, N), 0.3, 3.0, ((0, 4), (1, 8)), jnp.float32)
    group_ids = draw_group_ids(jax.random.fold_in(key_list[6], 71), 0)
    return {"gradient": gradient, "eigenbasis": eigenbasis, "first_moment": first_moment, "second_moment": second_moment, "prior_update": prior_update, "group_ids": group_ids}


beta_one = 0.9
beta_two = 0.95
correct_one = 1.0 - 0.9 ** 10
correct_two = 1.0 - 0.95 ** 10
epsilon = 1e-08

def reference(gradient, eigenbasis, first_moment, second_moment, prior_update, group_ids):
    grad_float = gradient.astype(jnp.float32)
    update = prior_update
    firsts = []
    seconds = []
    for group_slot in range(GROUPS):
        begin = (group_ids[group_slot] * GROUP).astype(jnp.int32)
        group_basis = lax.dynamic_slice_in_dim(eigenbasis, begin, GROUP, 1)
        rotated = jnp.dot(group_basis.T, grad_float, precision=lax.Precision.HIGHEST, preferred_element_type=jnp.float32)
        moment_one = beta_one * first_moment[group_slot] + (1.0 - beta_one) * rotated
        moment_two = beta_two * second_moment[group_slot] + (1.0 - beta_two) * rotated * rotated
        adjusted = moment_one / correct_one / (jnp.sqrt(moment_two / correct_two) + epsilon)
        update = update + jnp.dot(group_basis, adjusted, precision=lax.Precision.HIGHEST, preferred_element_type=jnp.float32)
        firsts.append(moment_one)
        seconds.append(moment_two)
    return (jnp.stack(firsts), jnp.stack(seconds), update)
```

```python
import jax
import jax.numpy as jnp
from jax import lax
from jax.sharding import PartitionSpec as P

GROUP = 256
GROUPS = 4
EARLY = 2


beta_one = 0.9
beta_two = 0.95
correct_one = 1.0 - 0.9**10
correct_two = 1.0 - 0.95**10
epsilon = 1e-08


def cut(x, index, count, axis=0):
    return lax.dynamic_slice_in_dim(x, index * count, count, axis)


def own_columns(eigenbasis, group_index):
    width = eigenbasis.shape[1]
    begin = group_index * GROUP - lax.axis_index("cols") * width
    if width >= GROUP:
        held = jnp.logical_and(begin >= 0, begin < width)
        block = lax.dynamic_slice_in_dim(eigenbasis, jnp.where(held, begin, 0), GROUP, 1)
        return jnp.where(held, block, jnp.zeros_like(block))
    held = jnp.logical_and(begin <= 0, begin > -GROUP)
    place = jnp.where(held, -begin, 0)
    block = jnp.where(held, eigenbasis, jnp.zeros_like(eigenbasis))
    empty = jnp.zeros((eigenbasis.shape[0], GROUP), eigenbasis.dtype)
    return lax.dynamic_update_slice_in_dim(empty, block, place, 1)


def halves(x):
    high = lax.reduce_precision(x, 8, 7)
    return high.astype(jnp.bfloat16), (x - high).astype(jnp.bfloat16)


def swap(x, bit):
    return lax.ppermute(x, "rows", [(i, i ^ bit) for i in range(lax.axis_size("rows"))])


def rotate(high, low, gradient):
    count = high.shape[1]
    both = lax.dot_general(
        jnp.concatenate([high, low], axis=1),
        gradient,
        (((0,), (0,)), ((), ())),
        preferred_element_type=jnp.float32,
    )
    return both[:count] + both[count:]


def rotated_share(high, low, gradient, rows_here):
    row = lax.axis_index("rows")
    far, core = row // 2, row % 2

    def chip_sum(half):
        part = rotate(
            cut(high, half, 2 * rows_here, 1), cut(low, half, 2 * rows_here, 1), gradient
        )
        return cut(part, core, rows_here) + swap(cut(part, 1 - core, rows_here), 1)

    away = swap(chip_sum(1 - far), 2)
    return chip_sum(far) + away


def share_all(x):
    row = lax.axis_index("rows")
    far, core = row // 2, row % 2
    rows_here = x.shape[0]
    other = swap(x, 2)
    first = far == 0
    mine = jnp.concatenate([jnp.where(first, x, other), jnp.where(first, other, x)])
    theirs = swap(mine, 1)
    first = core == 0
    even = jnp.where(first, mine, theirs)
    odd = jnp.where(first, theirs, mine)
    return jnp.concatenate(
        [even[:rows_here], odd[:rows_here], even[rows_here:], odd[rows_here:]]
    )


def per_device(gradient, eigenbasis, first_moment, second_moment, prior_update, group_ids):
    rows_here = first_moment.shape[1]
    blocks = [own_columns(eigenbasis, group_ids[slot]) for slot in range(GROUPS)]
    early, late = (jnp.concatenate(part, axis=1) for part in (blocks[:EARLY], blocks[EARLY:]))
    early = lax.psum(early, "cols")
    early, late = lax.optimization_barrier((early, late))
    late = lax.psum(late, "cols")
    update = prior_update
    firsts = []
    seconds = []
    for batch in (range(EARLY), range(EARLY, GROUPS)):
        if batch[0] == EARLY:
            late, update = lax.optimization_barrier((late, update))
        bases = []
        adjusts = []
        for slot in batch:
            basis = cut(early if slot < EARLY else late, slot - batch[0], GROUP, 1)
            high, low = halves(basis)
            rotated = rotated_share(high, low, gradient, rows_here)
            old_one, old_two = lax.optimization_barrier((first_moment[slot], second_moment[slot]))
            moment_one = beta_one * old_one + (1.0 - beta_one) * rotated
            moment_two = beta_two * old_two + (1.0 - beta_two) * rotated * rotated
            adjusts.append(
                moment_one / correct_one / (jnp.sqrt(moment_two / correct_two) + epsilon)
            )
            bases.append((high, low))
            firsts.append(moment_one)
            seconds.append(moment_two)
        lefts = []
        rights = []
        for (high, low), adjusted in zip(bases, adjusts):
            whole_high, whole_low = halves(share_all(adjusted))
            lefts += [high, high, low]
            rights += [whole_high, whole_low, whole_high]
        update = update + jnp.dot(
            jnp.concatenate(lefts, axis=1),
            jnp.concatenate(rights, axis=0),
            preferred_element_type=jnp.float32,
        )
    return (jnp.stack(firsts), jnp.stack(seconds), update)


def solution(mesh):
    placed = (
        P("rows", "cols"),
        P("rows", "cols"),
        P(None, "rows", "cols"),
        P(None, "rows", "cols"),
        P("rows", "cols"),
        P(),
    )
    return jax.shard_map(
        per_device,
        mesh=mesh,
        in_specs=placed,
        out_specs=(P(None, "rows", "cols"), P(None, "rows", "cols"), P("rows", "cols")),
        check_vma=False,
    )
```
